64 devices in a mesh: dp: 8 (over x, y, core), sp: 8 (over z).
Axes of the slice: x: 2, y: 2, z: 8, core: 2. Of those that a mesh axis runs over, the one named last changes fastest.
The devices are a block of a 4x4x8 slice.
Arguments:
- q: bfloat16 [256, 24, 128], P('dp'), parts along dimension 0
- k: bfloat16 [256, 4096, 8, 128], P('dp', 'sp'), parts along dimension 0
- v: bfloat16 [256, 4096, 8, 128], P('dp', 'sp'), parts along dimension 0
Outputs:
- q: bfloat16 [256, 24, 128], P('dp'), parts along dimension 0
There are 8 independent parts. The reference program is written for one: setup_inputs(seed, part) draws one part's arguments, and reference() takes and returns one part's arrays. A program takes and returns all parts, laid end to end along the dimension named above; each array names one.
All inputs are finite; a program needn't handle non-finite values.
Results may differ from the reference program's by a relative error of at most 0.012.
Values are sent between devices in bfloat16 or wider.
A program may use at most 768 MiB of HBM per device.

```python
import jax
import jax.numpy as jnp

BATCH = 32
CACHE = 4096
HEADS = 24
KV_HEADS = 8
HEAD = 128


def setup_inputs(seed: int = 0, part: int = 0) -> dict:
    kq, kk, kv = (jax.random.fold_in(k, part) for k in jax.random.split(jax.random.key(seed), 3))
    return {
        "q": (3 * jax.random.normal(kq, (BATCH, HEADS, HEAD), jnp.float32)).astype(jnp.bfloat16),
        "k": jax.random.normal(kk, (BATCH, CACHE, KV_HEADS, HEAD), jnp.float32).astype(jnp.bfloat16),
        "v": jax.random.normal(kv, (BATCH, CACHE, KV_HEADS, HEAD), jnp.float32).astype(jnp.bfloat16),
    }


def einsum(form, a, b):
    return jnp.einsum(form, a.astype(jnp.float32), b.astype(jnp.float32))


def reference(q, k, v):
    grouped = q.reshape(BATCH, KV_HEADS, -1, HEAD)
    scores = einsum("bgsd,bugd->bgsu", grouped, k) * HEAD**-0.5
    weights = jax.nn.softmax(scores, -1).astype(jnp.bfloat16)
    return einsum("bgsu,bugd->bgsd", weights, v).astype(jnp.bfloat16).reshape(BATCH, HEADS, HEAD)
```

```python
import functools
import math

import jax
import jax.numpy as jnp
from jax import lax
from jax.experimental import pallas as pl
from jax.experimental.pallas import tpu as pltpu
from jax.sharding import PartitionSpec as P

LANES = 128
SIDE = 256
SLOTS = 8
SUMS = 32


def attend(q_ref, k_hbm, v_hbm, out_ref, kbuf, vbuf, scores, highs, part, stat, parts, stats,
           k_sem, v_sem, part_out, stat_out, part_in, stat_in, res_out, res_in, *, n, heads_per):
    batch, heads, head = q_ref.shape
    rows = k_hbm.shape[1]
    tiles = rows // (2 * SIDE)
    key_heads = heads // heads_per
    rounds = batch // n
    factor = head**-0.5 * math.log2(math.e)
    me = lax.axis_index("sp")

    def seq_of(p):
        step = p % n
        half = (step + 1) // 2
        return (p // n) * n + (me + n // 2 + (1 - 2 * (step % 2)) * half + n) % n

    def owner_of(p):
        step = p % n
        half = (step + 1) // 2
        return (me + n // 2 + (1 - 2 * (step % 2)) * half + n) % n

    def fetch_k(p):
        return pltpu.make_async_copy(k_hbm.at[seq_of(p)], kbuf.at[p % SLOTS], k_sem.at[p % SLOTS])

    def fetch_v(p):
        return pltpu.make_async_copy(v_hbm.at[seq_of(p)], vbuf.at[p % SLOTS], v_sem.at[p % SLOTS])

    barrier = pltpu.get_barrier_semaphore()
    for hop in range(1, n):
        pl.semaphore_signal(barrier, inc=1, device_id={"sp": (me + hop) % n}, device_id_type=pl.DeviceIdType.MESH)
    fetch_k(0).start()
    for p in range(1, SLOTS):
        fetch_k(p).start()
        fetch_v(p - 1).start()
    fetch_v(SLOTS - 1).start()
    pl.semaphore_wait(barrier, n - 1)

    row = lax.broadcasted_iota(jnp.int32, (2 * heads, LANES), 0) % heads
    lane = lax.broadcasted_iota(jnp.int32, (2 * heads, LANES), 1)
    mine = row // heads_per == lane % key_heads
    diagonal = lax.broadcasted_iota(jnp.int32, (heads, LANES), 0) == lane[:heads]
    diagonal_sums = lax.broadcasted_iota(jnp.int32, (heads, LANES), 0) + SUMS == lane[:heads]

    def twice(ref, slot, tile):
        one = ref[slot, pl.ds(tile * 2 * SIDE, SIDE), :]
        other = ref[slot, pl.ds(tile * 2 * SIDE + SIDE, SIDE), :]
        return jnp.concatenate([one, other], 1)

    def queries(p):
        q = q_ref[seq_of(p)].astype(jnp.float32)
        zero = jnp.zeros_like(q)
        return jnp.concatenate([jnp.concatenate([q, zero], 1), jnp.concatenate([zero, q], 1)], 0).astype(jnp.bfloat16)

    def score_tile(p, both, tile, high):
        s = lax.dot_general(both, twice(kbuf, p % SLOTS, tile), (((1,), (1,)), ((), ())), preferred_element_type=jnp.float32)
        for half in range(SIDE // LANES):
            piece = jnp.where(mine, s[:, half * LANES:(half + 1) * LANES] * factor, -jnp.inf)
            scores[p % 2, tile, :, half * LANES:(half + 1) * LANES] = piece
            high = piece if high is None else jnp.maximum(high, piece)
        return high

    def score_end(p, high):
        high = jnp.maximum(high[:heads], high[heads:])
        highs[p % 2] = jnp.broadcast_to(jnp.max(high, 1, keepdims=True), (heads, LANES))

    def value_tile(p, high, tile, total, seen):
        weights = []
        for half in range(SIDE // LANES):
            w = jnp.exp2(scores[p % 2, tile, :, half * LANES:(half + 1) * LANES] - high)
            total = w if total is None else total + w
            weights.append(w)
        w = jnp.concatenate(weights, 1).astype(jnp.bfloat16)
        add = jnp.dot(w, twice(vbuf, p % SLOTS, tile), preferred_element_type=jnp.float32)
        return total, add if seen is None else seen + add

    def value_end(p, high, total, seen):
        seq = seq_of(p)
        part[seq] = (seen[:heads, :LANES] + seen[heads:, LANES:]).astype(jnp.bfloat16)
        total = jnp.sum(total[:heads] + total[heads:], 1, keepdims=True)
        stat[seq] = jnp.sum(jnp.where(diagonal, high, jnp.where(diagonal_sums, total, 0.0)), 0, keepdims=True)

    def send(p):
        seq = seq_of(p)
        turn = p // n

        @pl.when(p % n < n - 1)
        def _():
            to = {"sp": owner_of(p)}
            pltpu.make_async_remote_copy(part.at[seq], parts.at[turn, me], part_out, part_in.at[turn], device_id=to, device_id_type=pl.DeviceIdType.MESH).start()
            pltpu.make_async_remote_copy(stat.at[seq], stats.at[turn, me], stat_out, stat_in.at[turn], device_id=to, device_id_type=pl.DeviceIdType.MESH).start()

        @pl.when(p % n == n - 1)
        def _():
            parts[turn, me] = part[seq]
            stats[turn, me] = stat[seq]

    def together(turn):
        pltpu.make_async_copy(parts.at[turn, pl.ds(0, n - 1)], parts.at[turn, pl.ds(0, n - 1)], part_in.at[turn]).wait()
        pltpu.make_async_copy(stats.at[turn, pl.ds(0, n - 1)], stats.at[turn, pl.ds(0, n - 1)], stat_in.at[turn]).wait()
        known = stats[turn].reshape(n, LANES)
        scale = jnp.exp2(known - jnp.max(known, 0, keepdims=True))
        sums = pltpu.roll(known, LANES - SUMS, 1)
        scale = scale / jnp.sum(scale * sums, 0, keepdims=True)
        result = None
        for device in range(n):
            own = jnp.sum(jnp.where(diagonal, jnp.broadcast_to(scale[device:device + 1], (heads, LANES)), 0.0), 1, keepdims=True)
            term = parts[turn, device].astype(jnp.float32) * own
            result = term if result is None else result + term
        seq = turn * n + me
        out_ref[seq] = result.astype(out_ref.dtype)
        for hop in range(1, n):
            to = {"sp": (me + (n // 2 + (1 - 2 * (hop % 2)) * (hop // 2) + n) % n) % n}
            pltpu.make_async_remote_copy(out_ref.at[seq], out_ref.at[seq], res_out, res_in, device_id=to, device_id_type=pl.DeviceIdType.MESH).start()

    fetch_k(0).wait()
    both = queries(0)
    high = None
    for tile in range(tiles):
        high = score_tile(0, both, tile, high)
    score_end(0, high)
    if batch > SLOTS:
        fetch_k(SLOTS).start()

    def step(p, _):
        fetch_k(p).wait()
        fetch_v(p - 1).wait()
        both = queries(p)
        last = highs[(p - 1) % 2]
        last_twice = jnp.concatenate([last, last], 0)
        high = total = seen = None
        for tile in range(tiles):
            high = score_tile(p, both, tile, high)
            total, seen = value_tile(p - 1, last_twice, tile, total, seen)
        score_end(p, high)
        value_end(p - 1, last, total, seen)

        @pl.when(p + SLOTS < batch)
        def _():
            fetch_k(p + SLOTS).start()

        @pl.when(p - 1 + SLOTS < batch)
        def _():
            fetch_v(p - 1 + SLOTS).start()

        send(p - 1)

        @pl.when((p > n) & (p % n == n // 2))
        def _():
            together(p // n - 1)

        return 0

    lax.fori_loop(1, batch, step, 0)
    fetch_v(batch - 1).wait()
    last = highs[(batch - 1) % 2]
    last_twice = jnp.concatenate([last, last], 0)
    total = seen = None
    for tile in range(tiles):
        total, seen = value_tile(batch - 1, last_twice, tile, total, seen)
    value_end(batch - 1, last, total, seen)
    send(batch - 1)
    together(rounds - 1)

    away = batch - rounds
    pltpu.make_async_copy(out_ref.at[pl.ds(0, away)], out_ref.at[pl.ds(0, away)], res_in).wait()
    pltpu.make_async_copy(out_ref.at[pl.ds(0, away)], out_ref.at[pl.ds(0, away)], res_out).wait()
    pltpu.make_async_copy(part.at[pl.ds(0, away)], part.at[pl.ds(0, away)], part_out).wait()
    pltpu.make_async_copy(stat.at[pl.ds(0, away)], stat.at[pl.ds(0, away)], stat_out).wait()


def solution(mesh):
    n = mesh.shape["sp"]

    def step(q, k, v):
        batch, heads, head = q.shape
        tokens, key_heads = k.shape[1:3]
        rows = tokens * key_heads
        rounds = batch // n
        vmem = pltpu.VMEM
        return pl.pallas_call(
            functools.partial(attend, n=n, heads_per=heads // key_heads),
            out_shape=jax.ShapeDtypeStruct(q.shape, q.dtype),
            in_specs=[pl.BlockSpec(memory_space=vmem), pl.BlockSpec(memory_space=pl.ANY), pl.BlockSpec(memory_space=pl.ANY)],
            out_specs=pl.BlockSpec(memory_space=vmem),
            scratch_shapes=[
                vmem((SLOTS, rows, head), k.dtype),
                vmem((SLOTS, rows, head), v.dtype),
                vmem((2, rows // (2 * SIDE), 2 * heads, SIDE), jnp.float32),
                vmem((2, heads, LANES), jnp.float32),
                vmem((batch, heads, head), q.dtype),
                vmem((batch, 1, LANES), jnp.float32),
                vmem((rounds, n, heads, head), q.dtype),
                vmem((rounds, n, 1, LANES), jnp.float32),
                pltpu.SemaphoreType.DMA((SLOTS,)),
                pltpu.SemaphoreType.DMA((SLOTS,)),
                pltpu.SemaphoreType.DMA(()),
                pltpu.SemaphoreType.DMA(()),
                pltpu.SemaphoreType.DMA((rounds,)),
                pltpu.SemaphoreType.DMA((rounds,)),
                pltpu.SemaphoreType.DMA(()),
                pltpu.SemaphoreType.DMA(()),
            ],
            compiler_params=pltpu.CompilerParams(collective_id=0, has_side_effects=True, vmem_limit_bytes=60 * 1024 * 1024),
            name="attend",
        )(q, k.reshape(batch, rows, head), v.reshape(batch, rows, head))

    return jax.shard_map(
        step,
        mesh=mesh,
        in_specs=(P("dp", None, None), P("dp", "sp", None, None), P("dp", "sp", None, None)),
        out_specs=P("dp", None, None),
        check_vma=False,
    )
```

```python
import functools
import math

import jax
import jax.numpy as jnp
from jax import lax
from jax.experimental import pallas as pl
from jax.experimental.pallas import tpu as pltpu
from jax.sharding import PartitionSpec as P

LANES = 128
SIDE = 256
SLOTS = 8
GROUP = 16
SUMS = 32


def attend(q_hbm, k_hbm, v_hbm, out_ref, q_ref, kbuf, vbuf, scores, highs, part, stat, parts, stats,
           q_sem, k_sem, v_sem, part_out, stat_out, part_in, stat_in, res_out, res_in, *, n, heads_per):
    batch, heads, head = q_ref.shape
    rows = k_hbm.shape[1]
    tiles = rows // (2 * SIDE)
    key_heads = heads // heads_per
    rounds = batch // n
    factor = head**-0.5 * math.log2(math.e)
    me = lax.axis_index("sp")

    def seq_of(p):
        step = p % n
        half = (step + 1) // 2
        return (p // n) * n + (me + n // 2 + (1 - 2 * (step % 2)) * half + n) % n

    def owner_of(p):
        step = p % n
        half = (step + 1) // 2
        return (me + n // 2 + (1 - 2 * (step % 2)) * half + n) % n

    def fetch_k(p):
        return pltpu.make_async_copy(k_hbm.at[seq_of(p)], kbuf.at[p % SLOTS], k_sem.at[p % SLOTS])

    def fetch_v(p):
        return pltpu.make_async_copy(v_hbm.at[seq_of(p)], vbuf.at[p % SLOTS], v_sem.at[p % SLOTS])

    scope = jax.named_scope
    fetch_q = pltpu.make_async_copy(q_hbm, q_ref, q_sem)
    fetch_k(0).start()
    fetch_q.start()
    for p in range(1, SLOTS):
        fetch_k(p).start()
        fetch_v(p - 1).start()
    fetch_v(SLOTS - 1).start()
    barrier = pltpu.get_barrier_semaphore()
    for hop in range(1, n):
        pl.semaphore_signal(barrier, inc=1, device_id={"sp": (me + hop) % n}, device_id_type=pl.DeviceIdType.MESH)

    row = lax.broadcasted_iota(jnp.int32, (2 * heads, LANES), 0) % heads
    lane = lax.broadcasted_iota(jnp.int32, (2 * heads, LANES), 1)
    mine = row // heads_per == lane % key_heads
    diagonal = lax.broadcasted_iota(jnp.int32, (heads, LANES), 0) == lane[:heads]
    diagonal_sums = lax.broadcasted_iota(jnp.int32, (heads, LANES), 0) + SUMS == lane[:heads]

    def twice(ref, slot, tile):
        groups = [ref[slot, pl.ds(tile * 2 * SIDE + first, GROUP), :] for first in range(0, 2 * SIDE, GROUP)]
        return jnp.concatenate([jnp.concatenate(groups[::2], 0), jnp.concatenate(groups[1::2], 0)], 1)

    def queries(p):
        q = q_ref[seq_of(p)].astype(jnp.float32)
        zero = jnp.zeros_like(q)
        return jnp.concatenate([jnp.concatenate([q, zero], 1), jnp.concatenate([zero, q], 1)], 0).astype(jnp.bfloat16)

    def score_tile(p, both, tile, high):
        s = lax.dot_general(both, twice(kbuf, p % SLOTS, tile), (((1,), (1,)), ((), ())), preferred_element_type=jnp.float32)
        for half in range(SIDE // LANES):
            piece = jnp.where(mine, s[:, half * LANES:(half + 1) * LANES] * factor, -jnp.inf)
            scores[p % 2, tile, :, half * LANES:(half + 1) * LANES] = piece
            high = piece if high is None else jnp.maximum(high, piece)
        return high

    def score_end(p, high):
        high = jnp.maximum(high[:heads], high[heads:])
        highs[p % 2] = jnp.broadcast_to(jnp.max(high, 1, keepdims=True), (heads, LANES))

    def value_tile(p, high, tile, total, seen):
        weights = []
        for half in range(SIDE // LANES):
            w = jnp.exp2(scores[p % 2, tile, :, half * LANES:(half + 1) * LANES] - high)
            total = w if total is None else total + w
            weights.append(w)
        w = jnp.concatenate(weights, 1).astype(jnp.bfloat16)
        add = jnp.dot(w, twice(vbuf, p % SLOTS, tile), preferred_element_type=jnp.float32)
        return total, add if seen is None else seen + add

    def value_end(p, high, total, seen):
        seq = seq_of(p)
        part[seq] = (seen[:heads, :LANES] + seen[heads:, LANES:]).astype(jnp.bfloat16)
        total = jnp.sum(total[:heads] + total[heads:], 1, keepdims=True)
        stat[seq] = jnp.sum(jnp.where(diagonal, high, jnp.where(diagonal_sums, total, 0.0)), 0, keepdims=True)

    def send(p):
        seq = seq_of(p)
        turn = p // n

        @pl.when(p % n < n - 1)
        def _():
            to = {"sp": owner_of(p)}
            pltpu.make_async_remote_copy(part.at[seq], parts.at[turn, me], part_out, part_in.at[turn], device_id=to, device_id_type=pl.DeviceIdType.MESH).start()
            pltpu.make_async_remote_copy(stat.at[seq], stats.at[turn, me], stat_out, stat_in.at[turn], device_id=to, device_id_type=pl.DeviceIdType.MESH).start()

        @pl.when(p % n == n - 1)
        def _():
            parts[turn, me] = part[seq]
            stats[turn, me] = stat[seq]

    def together(turn):
        with scope("wait_parts"):
            pltpu.make_async_copy(parts.at[turn, pl.ds(0, n - 1)], parts.at[turn, pl.ds(0, n - 1)], part_in.at[turn]).wait()
            pltpu.make_async_copy(stats.at[turn, pl.ds(0, n - 1)], stats.at[turn, pl.ds(0, n - 1)], stat_in.at[turn]).wait()
        known = stats[turn].reshape(n, LANES)
        scale = jnp.exp2(known - jnp.max(known, 0, keepdims=True))
        sums = pltpu.roll(known, LANES - SUMS, 1)
        scale = scale / jnp.sum(scale * sums, 0, keepdims=True)
        result = None
        for device in range(n):
            own = jnp.sum(jnp.where(diagonal, jnp.broadcast_to(scale[device:device + 1], (heads, LANES)), 0.0), 1, keepdims=True)
            term = parts[turn, device].astype(jnp.float32) * own
            result = term if result is None else result + term
        seq = turn * n + me
        out_ref[seq] = result.astype(out_ref.dtype)
        for hop in range(1, n):
            to = {"sp": (me + (n // 2 + (1 - 2 * (hop % 2)) * (hop // 2) + n) % n) % n}
            pltpu.make_async_remote_copy(out_ref.at[seq], out_ref.at[seq], res_out, res_in, device_id=to, device_id_type=pl.DeviceIdType.MESH).start()

    with scope("wait_k0"):
        fetch_q.wait()
        fetch_k(0).wait()
    both = queries(0)
    high = None
    for tile in range(tiles):
        high = score_tile(0, both, tile, high)
    score_end(0, high)
    if batch > SLOTS:
        fetch_k(SLOTS).start()

    held = n + n // 2
    first = batch - 2 - 3 * (rounds - 2)

    def step(p, _, sending):
        with scope("wait_k"):
            fetch_k(p).wait()
        with scope("wait_v"):
            fetch_v(p - 1).wait()
        both = queries(p)
        last = highs[(p - 1) % 2]
        last_twice = jnp.concatenate([last, last], 0)
        high = total = seen = None
        for tile in range(tiles):
            high = score_tile(p, both, tile, high)
            total, seen = value_tile(p - 1, last_twice, tile, total, seen)
        score_end(p, high)
        value_end(p - 1, last, total, seen)

        @pl.when(p + SLOTS < batch)
        def _():
            fetch_k(p + SLOTS).start()

        @pl.when(p - 1 + SLOTS < batch)
        def _():
            fetch_v(p - 1 + SLOTS).start()

        if sending:
            send(p - 1)

            @pl.when((p >= first) & ((p - first) % 3 == 0))
            def _():
                together((p - first) // 3)

        return 0

    def send_held(p, _):
        send(p)
        return 0

    lax.fori_loop(1, held + 1, functools.partial(step, sending=False), 0)
    with scope("barrier"):
        pl.semaphore_wait(barrier, n - 1)
    with scope("send_held"):
        lax.fori_loop(0, held, send_held, 0)
    lax.fori_loop(held + 1, batch, functools.partial(step, sending=True), 0)
    with scope("wait_v_last"):
        fetch_v(batch - 1).wait()
    last = highs[(batch - 1) % 2]
    last_twice = jnp.concatenate([last, last], 0)
    total = seen = None
    for tile in range(tiles):
        total, seen = value_tile(batch - 1, last_twice, tile, total, seen)
    value_end(batch - 1, last, total, seen)
    send(batch - 1)
    with scope("together_last"):
        together(rounds - 1)

    away = batch - rounds
    rest = scope("wait_results")
    rest.__enter__()
    pltpu.make_async_copy(out_ref.at[pl.ds(0, away)], out_ref.at[pl.ds(0, away)], res_in).wait()
    pltpu.make_async_copy(out_ref.at[pl.ds(0, away)], out_ref.at[pl.ds(0, away)], res_out).wait()
    pltpu.make_async_copy(part.at[pl.ds(0, away)], part.at[pl.ds(0, away)], part_out).wait()
    pltpu.make_async_copy(stat.at[pl.ds(0, away)], stat.at[pl.ds(0, away)], stat_out).wait()
    rest.__exit__(None, None, None)


def solution(mesh):
    n = mesh.shape["sp"]

    def step(q, k, v):
        batch, heads, head = q.shape
        tokens, key_heads = k.shape[1:3]
        rows = tokens * key_heads
        rounds = batch // n
        vmem = pltpu.VMEM
        return pl.pallas_call(
            functools.partial(attend, n=n, heads_per=heads // key_heads),
            out_shape=jax.ShapeDtypeStruct(q.shape, q.dtype),
            in_specs=[pl.BlockSpec(memory_space=pl.ANY), pl.BlockSpec(memory_space=pl.ANY), pl.BlockSpec(memory_space=pl.ANY)],
            out_specs=pl.BlockSpec(memory_space=vmem),
            scratch_shapes=[
                vmem(q.shape, q.dtype),
                vmem((SLOTS, rows, head), k.dtype),
                vmem((SLOTS, rows, head), v.dtype),
                vmem((2, rows // (2 * SIDE), 2 * heads, SIDE), jnp.float32),
                vmem((2, heads, LANES), jnp.float32),
                vmem((batch, heads, head), q.dtype),
                vmem((batch, 1, LANES), jnp.float32),
                vmem((rounds, n, heads, head), q.dtype),
                vmem((rounds, n, 1, LANES), jnp.float32),
                pltpu.SemaphoreType.DMA(()),
                pltpu.SemaphoreType.DMA((SLOTS,)),
                pltpu.SemaphoreType.DMA((SLOTS,)),
                pltpu.SemaphoreType.DMA(()),
                pltpu.SemaphoreType.DMA(()),
                pltpu.SemaphoreType.DMA((rounds,)),
                pltpu.SemaphoreType.DMA((rounds,)),
                pltpu.SemaphoreType.DMA(()),
                pltpu.SemaphoreType.DMA(()),
            ],
            compiler_params=pltpu.CompilerParams(collective_id=0, has_side_effects=True, vmem_limit_bytes=60 * 1024 * 1024),
            name="attend",
        )(q, k.reshape(batch, rows, head), v.reshape(batch, rows, head))

    return jax.shard_map(
        step,
        mesh=mesh,
        in_specs=(P("dp", None, None), P("dp", "sp", None, None), P("dp", "sp", None, None)),
        out_specs=P("dp", None, None),
        check_vma=False,
    )
```
